32 devices in a mesh: row: 16 (over z, x, core), col: 2 (over y).
Axes of the slice: x: 2, y: 2, z: 4, core: 2. Of those that a mesh axis runs over, the one named last changes fastest.
Arguments:
- species: float32 [2, 128, 128, 64], P(None, None, 'row', 'col'), may hold values from -6 to 6
- symbol_x: float32 [128], replicated, may hold values from 0.3 to 3
- symbol_y: float32 [128], replicated, may hold values from 0.3 to 3
- symbol_z: float32 [64], replicated, may hold values from 0.3 to 3
Outputs:
- spectrum: float32 [2, 128, 128, 64], P(None, 'row', 'col')
The draws below stay inside these ranges and needn't reach their ends.
All inputs are finite; a program needn't handle non-finite values.
Results may differ from the reference program's by a relative error of at most 0.00007.
Values sent between devices are 32-bit elements; how exact they have to be, the bound alone decides.
A program may use at most 64 MiB of HBM per device.

```python
import jax
import jax.numpy as jnp
from jax import lax

GRID_X = 128
GRID_Y = 128
GRID_Z = 64
FIELDS = 2


def level_of(own_key, extent, split, least, high):
    def one(position, shards_of):
        heights = jax.random.uniform(jax.random.fold_in(jax.random.fold_in(own_key, 6), position), (shards_of,), jnp.float32, least / len(split), high / len(split))
        return jnp.repeat(jnp.exp(heights), extent[position] // shards_of).reshape((-1,) + (1,) * (len(extent) - position - 1))

    level = one(*split[0])
    for cut in split[1:]:
        level = level * one(*cut)
    return level


def centred(rng, shape, scale, most, cuts=(), held_as=jnp.bfloat16):
    entries = jax.random.normal(rng, shape, jnp.float32) * scale
    if len(cuts) > 0:
        entries = level_of(rng, shape, cuts, -0.22, 0.18) * entries
    return jnp.clip(entries, min=-most, max=most).astype(held_as)


def setup_inputs(seed: int = 0) -> dict:
    key_of = jax.random.split(jax.random.key(seed), 5)
    return {
        "species": centred(key_of[0], (FIELDS, GRID_X, GRID_Y, GRID_Z), 1.0, 6.0, ((2, 16), (3, 2)), jnp.float32),
        "symbol_x": jnp.clip(jax.random.uniform(key_of[1], (GRID_X,), jnp.float32, 0.3, 3.0), 0.3, 3.0),
        "symbol_y": jnp.clip(jax.random.uniform(key_of[2], (GRID_Y,), jnp.float32, 0.3, 3.0), 0.3, 3.0),
        "symbol_z": jnp.clip(jax.random.uniform(key_of[3], (GRID_Z,), jnp.float32, 0.3, 3.0), 0.3, 3.0),
    }


def basis_table(count):
    rank = jnp.arange(count)
    angle = (jnp.pi / (4 * count)) * (((2 * rank[:, None] + 1) * (2 * rank[None, :] + 1)) % (8 * count)).astype(jnp.float32)
    return jnp.cos(angle) * (2.0 / count) ** 0.5


def to_modes(values, dim):
    moved = jnp.tensordot(values, basis_table(values.shape[dim]), axes=([dim], [0]), precision=lax.Precision.HIGHEST)
    return jnp.moveaxis(moved, -1, dim)


def reference(species, symbol_x, symbol_y, symbol_z):
    spectrum = species
    spectrum = to_modes(spectrum, 1)
    spectrum = to_modes(spectrum, 2)
    spectrum = to_modes(spectrum, 3)
    symbol = symbol_x[:, None, None] + symbol_y[None, :, None] + symbol_z[None, None, :]
    spectrum = spectrum / symbol
    return spectrum
```

```python
import functools

import jax
import jax.numpy as jnp
import ml_dtypes
import numpy as np
from jax import lax
from jax.experimental import pallas as pl
from jax.experimental.pallas import tpu as pltpu
from jax.sharding import PartitionSpec as P

LANES = 128
CUTS = 2
F32, BF16 = jnp.float32, jnp.bfloat16


def basis_table(count):
    odd = 2 * np.arange(count) + 1
    angle = np.pi / (4 * count) * (odd[:, None] * odd[None, :] % (8 * count))
    return np.cos(angle) * (2.0 / count) ** 0.5


def halves(table):
    high = table.astype(ml_dtypes.bfloat16)
    low = (table - high.astype(np.float64)).astype(ml_dtypes.bfloat16)
    return high, low


def split(values):
    high = values.astype(BF16)
    low = (values - high.astype(F32)).astype(BF16)
    return high, low


def tables(nx, ny, nz, share_z):
    width = LANES // share_z
    lane = np.arange(nx)
    group, rest = lane // LANES, lane % LANES
    order = width * (group * share_z + rest % share_z) + rest // share_z
    high, low = halves(basis_table(nx)[:, order])
    table_x = np.block([[high, low], [high, low]])
    high, low = halves(basis_table(ny))
    table_y = np.block([[high, high], [low, low]])
    eye = np.eye(width)
    wide = np.concatenate(
        [np.kron(eye, part) for part in np.split(basis_table(nz), nz // share_z, axis=0)], axis=0
    )
    table_z = np.stack(halves(wide))
    return table_x, table_y, table_z


def kernel(
    rows, cols, names,
    species, hx_hbm, hy_hbm, wz_hbm, sx_hbm, sy_hbm, sz_hbm,
    out,
    xin, hx, hy, wz, sx, sy, sz, send, recv, mixed, lines, tall_x, tall_y, scale,
    in_sem, row_send, row_recv, col_send, col_recv,
):
    row_name, col_name = names
    fields, share_y, share_z, nx = species.shape
    ny = rows * share_y
    nz = sz.shape[1]
    share_x, half_y = nx // rows, ny // cols
    width = LANES // share_z
    quads = share_x // width
    wide = quads * LANES // CUTS
    me, my_col = lax.axis_index(row_name), lax.axis_index(col_name)

    barrier = pltpu.get_barrier_semaphore()
    for k in range(1, rows):
        pl.semaphore_signal(
            barrier, inc=1, device_id={row_name: (me + k) % rows},
            device_id_type=pl.DeviceIdType.MESH,
        )
    for k in range(1, cols):
        pl.semaphore_signal(
            barrier, inc=1, device_id={col_name: (my_col + k) % cols},
            device_id_type=pl.DeviceIdType.MESH,
        )

    loads = [pltpu.make_async_copy(species.at[f], xin.at[f], in_sem.at[f]) for f in range(fields)]
    pairs = ((hx_hbm, hx), (hy_hbm, hy), (wz_hbm, wz), (sx_hbm, sx), (sy_hbm, sy), (sz_hbm, sz))
    fetches = [
        pltpu.make_async_copy(a, b, in_sem.at[fields + i]) for i, (a, b) in enumerate(pairs)
    ]
    loads[0].start()
    fetches[0].start()
    for copy in loads[1:] + fetches[1:]:
        copy.start()

    lane = lax.broadcasted_iota(jnp.int32, (share_y, LANES), 1)
    order = sorted(range(1, rows), key=lambda k: -min(k, rows - k))

    def row_copy(piece, target, origin):
        return pltpu.make_async_remote_copy(
            src_ref=send.at[piece, target],
            dst_ref=recv.at[piece, origin],
            send_sem=row_send.at[piece, target],
            recv_sem=row_recv.at[piece, origin],
            device_id={row_name: target},
            device_id_type=pl.DeviceIdType.MESH,
        )

    def col_copy(piece, target, origin):
        return pltpu.make_async_remote_copy(
            src_ref=mixed.at[piece, target],
            dst_ref=lines.at[piece, origin],
            send_sem=col_send.at[piece, target],
            recv_sem=col_recv.at[piece, origin],
            device_id={col_name: target},
            device_id_type=pl.DeviceIdType.MESH,
        )

    for f in range(fields):
        loads[f].wait()
        if f == 0:
            fetches[0].wait()
        high, low = split(
            jnp.concatenate(
                [xin[f, :, z, :] for z in range(share_z)], axis=0
            )
        )
        both = jnp.dot(
            jnp.concatenate([high, low], axis=1), hx[...], preferred_element_type=F32
        )
        both = both[:, :nx] + both[:, nx:]
        for group in range(nx // LANES):
            tiles = [
                both[z * share_y : (z + 1) * share_y, group * LANES : (group + 1) * LANES]
                for z in range(share_z)
            ]
            bit = 1
            while bit < share_z:
                keep = (lane & bit) == 0
                for i in range(share_z):
                    if i & bit == 0:
                        a, b = tiles[i], tiles[i + bit]
                        tiles[i] = jnp.where(keep, a, pltpu.roll(b, bit, 1))
                        tiles[i + bit] = jnp.where(keep, pltpu.roll(a, LANES - bit, 1), b)
                bit *= 2
            for i in range(share_z):
                q = group * share_z + i
                target, at = q // quads, q % quads * LANES
                send[f * CUTS + at // wide, target, :, at % wide : at % wide + LANES] = tiles[i]
        if f == 0:
            pl.semaphore_wait(barrier, rows + cols - 2)
        for cut in range(CUTS):
            piece = f * CUTS + cut
            for k in order:
                row_copy(piece, (me + k) % rows, me).start()
            recv[piece, me] = send[piece, me]

    for copy in fetches[1:]:
        copy.wait()
    tall_x[...] = jnp.broadcast_to(sx[...], (LANES, nx)).T
    tall_y[...] = jnp.broadcast_to(sy[...], (LANES, ny)).T
    part_y = tall_y[pl.ds(my_col * half_y, half_y), :1]
    for x in range(share_x):
        part_x = tall_x[pl.ds(me * share_x + x, 1), :1]
        at = x % width * nz
        scale[x // width, :, at : at + nz] = 1.0 / (part_x + part_y + sz[...])

    for piece in range(fields * CUTS):
        for k in order:
            origin = (me + rows - k) % rows
            row_copy(piece, origin, origin).wait_recv()
        high, low = split(recv[piece].reshape(ny, wide))
        both = jnp.dot(
            hy[...], jnp.concatenate([high, low], axis=0), preferred_element_type=F32
        )
        both = both[:ny] + both[ny:]
        mixed[piece] = both.reshape(cols, half_y, wide)
        for k in range(1, cols):
            col_copy(piece, (my_col + k) % cols, my_col).start()
        lines[piece, my_col] = mixed[piece, my_col]

    for piece in range(fields * CUTS):
        for k in range(1, cols):
            origin = (my_col + cols - k) % cols
            col_copy(piece, origin, origin).wait_recv()
        f, cut = piece // CUTS, piece % CUTS
        for i in range(wide // LANES):
            quad = cut * (wide // LANES) + i
            line = jnp.concatenate(
                [lines[piece, c, :, i * LANES : (i + 1) * LANES] for c in range(cols)], axis=1
            )
            high, low = split(line)
            both = jnp.dot(
                jnp.concatenate([high, low], axis=0), wz[0], preferred_element_type=F32
            )
            done = both[:half_y] + both[half_y:]
            done = done + jnp.dot(high, wz[1], preferred_element_type=F32)
            done = done * scale[quad]
            for j in range(width):
                out[f, quad * width + j] = done[:, j * nz : (j + 1) * nz]

    for piece in range(fields * CUTS):
        for k in order:
            row_copy(piece, (me + k) % rows, me).wait_send()
        for k in range(1, cols):
            col_copy(piece, (my_col + k) % cols, my_col).wait_send()


def on_device(rows, cols, species, symbol_x, symbol_y, symbol_z):
    fields, nx, share_y, share_z = species.shape
    ny, nz = symbol_y.shape[0], symbol_z.shape[0]
    share_x, half_y = nx // rows, ny // cols
    width = LANES // share_z
    pieces, wide = fields * CUTS, share_x // width * LANES // CUTS
    hx, hy, wz = (jnp.asarray(t) for t in tables(nx, ny, nz, share_z))
    dma = pltpu.SemaphoreType.DMA
    return pl.pallas_call(
        functools.partial(kernel, rows, cols, ("row", "col")),
        out_shape=jax.ShapeDtypeStruct((fields, share_x, half_y, nz), F32),
        in_specs=[pl.BlockSpec(memory_space=pl.ANY)] * 7,
        out_specs=pl.BlockSpec(memory_space=pltpu.VMEM),
        scratch_shapes=[
            pltpu.VMEM((fields, share_y, share_z, nx), F32),
            pltpu.VMEM(hx.shape, BF16),
            pltpu.VMEM(hy.shape, BF16),
            pltpu.VMEM(wz.shape, BF16),
            pltpu.VMEM((1, nx), F32),
            pltpu.VMEM((1, ny), F32),
            pltpu.VMEM((1, nz), F32),
            pltpu.VMEM((pieces, rows, share_y, wide), F32),
            pltpu.VMEM((pieces, rows, share_y, wide), F32),
            pltpu.VMEM((pieces, cols, half_y, wide), F32),
            pltpu.VMEM((pieces, cols, half_y, wide), F32),
            pltpu.VMEM((nx, LANES), F32),
            pltpu.VMEM((ny, LANES), F32),
            pltpu.VMEM((share_x // width, half_y, width * nz), F32),
            dma((fields + 6,)),
            dma((pieces, rows)),
            dma((pieces, rows)),
            dma((pieces, cols)),
            dma((pieces, cols)),
        ],
        compiler_params=pltpu.CompilerParams(collective_id=0, has_side_effects=True),
    )(
        jnp.transpose(species, (0, 2, 3, 1)), hx, hy, wz,
        symbol_x[None, :], symbol_y[None, :], symbol_z[None, :],
    )


def solution(mesh):
    rows, cols = mesh.shape["row"], mesh.shape["col"]
    in_specs = (P(None, None, "row", "col"), P(), P(), P())
    out_specs = P(None, "row", "col", None)
    return jax.shard_map(
        functools.partial(on_device, rows, cols),
        mesh=mesh, in_specs=in_specs, out_specs=out_specs, check_vma=False,
    )
```

```python
import functools

import jax
import jax.numpy as jnp
import ml_dtypes
import numpy as np
from jax import lax
from jax.experimental import pallas as pl
from jax.experimental.pallas import tpu as pltpu
from jax.sharding import PartitionSpec as P

LANES = 128
CUTS = 1
F32, BF16 = jnp.float32, jnp.bfloat16


def basis_table(count):
    odd = 2 * np.arange(count) + 1
    angle = np.pi / (4 * count) * (odd[:, None] * odd[None, :] % (8 * count))
    return np.cos(angle) * (2.0 / count) ** 0.5


def halves(table):
    high = table.astype(ml_dtypes.bfloat16)
    low = (table - high.astype(np.float64)).astype(ml_dtypes.bfloat16)
    return high, low


def split(values):
    high = values.astype(BF16)
    low = (values - high.astype(F32)).astype(BF16)
    return high, low


def tables(nx, ny, nz, share_z):
    width = LANES // share_z
    lane = np.arange(nx)
    group, rest = lane // LANES, lane % LANES
    order = width * (group * share_z + rest % share_z) + rest // share_z
    high, low = halves(basis_table(nx)[:, order])
    table_x = np.block([[high, low], [high, low]])
    high, low = halves(basis_table(ny))
    table_y = np.block([[high, high], [low, low]])
    eye = np.eye(width)
    wide = np.concatenate(
        [np.kron(eye, part) for part in np.split(basis_table(nz), nz // share_z, axis=0)], axis=0
    )
    table_z = np.stack(halves(wide))
    return table_x, table_y, table_z


def kernel(
    rows, cols, names,
    species, hx_hbm, hy_hbm, sx_hbm, sy_hbm, sz_hbm,
    lines, scale,
    xin, hx, hy, sx, sy, sz, send, recv, mixed, tall_x, tall_y,
    in_sem, row_send, row_recv, col_send, col_recv,
):
    row_name, col_name = names
    fields, share_y, share_z, nx = species.shape
    ny = rows * share_y
    nz = sz.shape[1]
    share_x, half_y = nx // rows, ny // cols
    width = LANES // share_z
    quads = share_x // width
    wide = quads * LANES // CUTS
    me, my_col = lax.axis_index(row_name), lax.axis_index(col_name)

    barrier = pltpu.get_barrier_semaphore()
    for k in range(1, rows):
        pl.semaphore_signal(
            barrier, inc=1, device_id={row_name: (me + k) % rows},
            device_id_type=pl.DeviceIdType.MESH,
        )
    for k in range(1, cols):
        pl.semaphore_signal(
            barrier, inc=1, device_id={col_name: (my_col + k) % cols},
            device_id_type=pl.DeviceIdType.MESH,
        )

    loads = [pltpu.make_async_copy(species.at[f], xin.at[f], in_sem.at[f]) for f in range(fields)]
    pairs = ((hx_hbm, hx), (hy_hbm, hy), (sx_hbm, sx), (sy_hbm, sy), (sz_hbm, sz))
    fetches = [
        pltpu.make_async_copy(a, b, in_sem.at[fields + i]) for i, (a, b) in enumerate(pairs)
    ]
    loads[0].start()
    fetches[0].start()
    for copy in loads[1:] + fetches[1:]:
        copy.start()

    lane = lax.broadcasted_iota(jnp.int32, (share_y, LANES), 1)
    order = sorted(range(1, rows), key=lambda k: -min(k, rows - k))

    def row_copy(piece, target, origin):
        return pltpu.make_async_remote_copy(
            src_ref=send.at[piece, target],
            dst_ref=recv.at[piece, origin],
            send_sem=row_send.at[piece, target],
            recv_sem=row_recv.at[piece, origin],
            device_id={row_name: target},
            device_id_type=pl.DeviceIdType.MESH,
        )

    def col_copy(piece, target, origin):
        return pltpu.make_async_remote_copy(
            src_ref=mixed.at[piece, target],
            dst_ref=lines.at[piece, origin],
            send_sem=col_send.at[piece, target],
            recv_sem=col_recv.at[piece, origin],
            device_id={col_name: target},
            device_id_type=pl.DeviceIdType.MESH,
        )

    for f in range(fields):
        loads[f].wait()
        if f == 0:
            fetches[0].wait()
        high, low = split(
            jnp.concatenate(
                [xin[f, :, z, :] for z in range(share_z)], axis=0
            )
        )
        both = jnp.dot(
            jnp.concatenate([high, low], axis=1), hx[...], preferred_element_type=F32
        )
        both = both[:, :nx] + both[:, nx:]
        for group in range(nx // LANES):
            tiles = [
                both[z * share_y : (z + 1) * share_y, group * LANES : (group + 1) * LANES]
                for z in range(share_z)
            ]
            bit = 1
            while bit < share_z:
                keep = (lane & bit) == 0
                for i in range(share_z):
                    if i & bit == 0:
                        a, b = tiles[i], tiles[i + bit]
                        tiles[i] = jnp.where(keep, a, pltpu.roll(b, bit, 1))
                        tiles[i + bit] = jnp.where(keep, pltpu.roll(a, LANES - bit, 1), b)
                bit *= 2
            for i in range(share_z):
                q = group * share_z + i
                target, at = q // quads, q % quads * LANES
                send[f * CUTS + at // wide, target, :, at % wide : at % wide + LANES] = tiles[i]
        if f == 0:
            pl.semaphore_wait(barrier, rows + cols - 2)
        for cut in range(CUTS):
            piece = f * CUTS + cut
            for k in order:
                row_copy(piece, (me + k) % rows, me).start()
            recv[piece, me] = send[piece, me]

    for copy in fetches[1:]:
        copy.wait()
    tall_x[...] = jnp.broadcast_to(sx[...], (LANES, nx)).T
    tall_y[...] = jnp.broadcast_to(sy[...], (LANES, ny)).T
    part_y = tall_y[pl.ds(my_col * half_y, half_y), :1]
    for x in range(share_x):
        part_x = tall_x[pl.ds(me * share_x + x, 1), :1]
        at = x % width * nz
        scale[x // width, :, at : at + nz] = 1.0 / (part_x + part_y + sz[...])

    for piece in range(fields * CUTS):
        for k in order:
            origin = (me + rows - k) % rows
            row_copy(piece, origin, origin).wait_recv()
        high, low = split(recv[piece].reshape(ny, wide))
        both = jnp.dot(
            hy[...], jnp.concatenate([high, low], axis=0), preferred_element_type=F32
        )
        both = both[:ny] + both[ny:]
        mixed[piece] = both.reshape(cols, half_y, wide)
        for k in range(1, cols):
            col_copy(piece, (my_col + k) % cols, my_col).start()
        lines[piece, my_col] = mixed[piece, my_col]

    for piece in range(fields * CUTS):
        for k in order:
            row_copy(piece, (me + k) % rows, me).wait_send()
        for k in range(1, cols):
            origin = (my_col + cols - k) % cols
            col_copy(piece, origin, origin).wait_recv()
            col_copy(piece, (my_col + k) % cols, my_col).wait_send()


def last_kernel(lines, scale, wz, out, held, out_sem):
    pieces, cols, half_y, wide = lines.shape
    nz = out.shape[3]
    width = scale.shape[2] // nz
    copies = []
    for piece in range(pieces):
        f, cut = piece // CUTS, piece % CUTS
        for i in range(wide // LANES):
            quad = cut * (wide // LANES) + i
            line = jnp.concatenate(
                [lines[piece, c, :, i * LANES : (i + 1) * LANES] for c in range(cols)], axis=1
            )
            high, low = split(line)
            both = jnp.dot(
                jnp.concatenate([high, low], axis=0), wz[0], preferred_element_type=F32
            )
            done = both[:half_y] + both[half_y:]
            done = done + jnp.dot(high, wz[1], preferred_element_type=F32)
            done = done * scale[quad]
            for j in range(width):
                held[f, quad * width + j] = done[:, j * nz : (j + 1) * nz]
            span = pl.ds(quad * width, width)
            copy = pltpu.make_async_copy(held.at[f, span], out.at[f, span], out_sem.at[f, quad])
            copy.start()
            copies.append(copy)
    for copy in copies:
        copy.wait()


def on_device(rows, cols, species, symbol_x, symbol_y, symbol_z):
    fields, nx, share_y, share_z = species.shape
    ny, nz = symbol_y.shape[0], symbol_z.shape[0]
    share_x, half_y = nx // rows, ny // cols
    width = LANES // share_z
    pieces, wide = fields * CUTS, share_x // width * LANES // CUTS
    hx, hy, wz = (jnp.asarray(t) for t in tables(nx, ny, nz, share_z))
    dma = pltpu.SemaphoreType.DMA
    width_z = width * nz
    vmem = pl.BlockSpec(memory_space=pltpu.VMEM)
    lines, scale = pl.pallas_call(
        functools.partial(kernel, rows, cols, ("row", "col")),
        out_shape=(
            jax.ShapeDtypeStruct((pieces, cols, half_y, wide), F32),
            jax.ShapeDtypeStruct((share_x // width, half_y, width_z), F32),
        ),
        in_specs=[pl.BlockSpec(memory_space=pl.ANY)] * 6,
        out_specs=(vmem, vmem),
        scratch_shapes=[
            pltpu.VMEM((fields, share_y, share_z, nx), F32),
            pltpu.VMEM(hx.shape, BF16),
            pltpu.VMEM(hy.shape, BF16),
            pltpu.VMEM((1, nx), F32),
            pltpu.VMEM((1, ny), F32),
            pltpu.VMEM((1, nz), F32),
            pltpu.VMEM((pieces, rows, share_y, wide), F32),
            pltpu.VMEM((pieces, rows, share_y, wide), F32),
            pltpu.VMEM((pieces, cols, half_y, wide), F32),
            pltpu.VMEM((nx, LANES), F32),
            pltpu.VMEM((ny, LANES), F32),
            dma((fields + 5,)),
            dma((pieces, rows)),
            dma((pieces, rows)),
            dma((pieces, cols)),
            dma((pieces, cols)),
        ],
        compiler_params=pltpu.CompilerParams(collective_id=0, has_side_effects=True, vmem_limit_bytes=16 * 2**20),
    )(
        *(pltpu.with_memory_space_constraint(v, pltpu.HBM) for v in (jnp.transpose(species, (0, 2, 3, 1)), hx, hy,
        symbol_x[None, :], symbol_y[None, :], symbol_z[None, :])),
    )
    shape = (fields, share_x, half_y, nz)
    return pl.pallas_call(
        last_kernel,
        out_shape=jax.ShapeDtypeStruct(shape, F32),
        in_specs=[vmem, vmem, vmem],
        out_specs=pl.BlockSpec(memory_space=pl.ANY),
        scratch_shapes=[pltpu.VMEM(shape, F32), dma((fields, share_x // width))],
        compiler_params=pltpu.CompilerParams(vmem_limit_bytes=16 * 2**20),
    )(lines, scale, wz)


def solution(mesh):
    rows, cols = mesh.shape["row"], mesh.shape["col"]
    in_specs = (P(None, None, "row", "col"), P(), P(), P())
    out_specs = P(None, "row", "col", None)
    return jax.shard_map(
        functools.partial(on_device, rows, cols),
        mesh=mesh, in_specs=in_specs, out_specs=out_specs, check_vma=False,
    )
```

```python
import functools

import jax
import jax.numpy as jnp
import ml_dtypes
import numpy as np
from jax import lax
from jax.experimental import pallas as pl
from jax.experimental.pallas import tpu as pltpu
from jax.sharding import PartitionSpec as P

LANES = 128
CUTS = 1
F32, BF16 = jnp.float32, jnp.bfloat16


def basis_table(count):
    odd = 2 * np.arange(count) + 1
    angle = np.pi / (4 * count) * (odd[:, None] * odd[None, :] % (8 * count))
    return np.cos(angle) * (2.0 / count) ** 0.5


def halves(table):
    high = table.astype(ml_dtypes.bfloat16)
    low = (table - high.astype(np.float64)).astype(ml_dtypes.bfloat16)
    return high, low


def split(values):
    high = values.astype(BF16)
    low = (values - high.astype(F32)).astype(BF16)
    return high, low


def tables(nx, ny, nz, share_z):
    width = LANES // share_z
    lane = np.arange(nx)
    group, rest = lane // LANES, lane % LANES
    order = width * (group * share_z + rest % share_z) + rest // share_z
    high, low = halves(basis_table(nx)[:, order])
    table_x = np.concatenate([high, low], axis=1)
    high, low = halves(basis_table(ny))
    table_y = np.block([[high, high], [low, low]])
    eye = np.eye(width)
    wide = np.concatenate(
        [np.kron(eye, part) for part in np.split(basis_table(nz), nz // share_z, axis=0)], axis=0
    )
    table_z = np.stack(halves(wide))
    return table_x, table_y, table_z


def kernel(
    rows, cols, names,
    species, hx_hbm, hy_hbm, sx_hbm, sy_hbm, sz_hbm,
    lines, scale,
    xin, hx, hy, sx, sy, sz, send, recv, mixed, tall_x, tall_y,
    in_sem, row_send, row_recv, col_send, col_recv,
):
    row_name, col_name = names
    fields, share_y, share_z, nx = species.shape
    ny = rows * share_y
    nz = sz.shape[1]
    share_x, half_y = nx // rows, ny // cols
    width = LANES // share_z
    quads = share_x // width
    wide = quads * LANES // CUTS
    me, my_col = lax.axis_index(row_name), lax.axis_index(col_name)

    barrier = pltpu.get_barrier_semaphore()
    for k in range(1, rows):
        pl.semaphore_signal(
            barrier, inc=1, device_id={row_name: (me + k) % rows},
            device_id_type=pl.DeviceIdType.MESH,
        )
    for k in range(1, cols):
        pl.semaphore_signal(
            barrier, inc=1, device_id={col_name: (my_col + k) % cols},
            device_id_type=pl.DeviceIdType.MESH,
        )

    loads = [pltpu.make_async_copy(species.at[f], xin.at[f], in_sem.at[f]) for f in range(fields)]
    pairs = ((hx_hbm, hx), (hy_hbm, hy), (sx_hbm, sx), (sy_hbm, sy), (sz_hbm, sz))
    fetches = [
        pltpu.make_async_copy(a, b, in_sem.at[fields + i]) for i, (a, b) in enumerate(pairs)
    ]
    loads[0].start()
    fetches[0].start()
    for copy in loads[1:]:
        copy.start()

    lane = lax.broadcasted_iota(jnp.int32, (share_y, LANES), 1)
    order = sorted(range(1, rows), key=lambda k: -min(k, rows - k))

    def row_copy(piece, target, origin):
        return pltpu.make_async_remote_copy(
            src_ref=send.at[piece, target],
            dst_ref=recv.at[piece, origin],
            send_sem=row_send.at[piece, target],
            recv_sem=row_recv.at[piece, origin],
            device_id={row_name: target},
            device_id_type=pl.DeviceIdType.MESH,
        )

    def col_copy(piece, target, origin):
        return pltpu.make_async_remote_copy(
            src_ref=mixed.at[piece, target],
            dst_ref=lines.at[piece, origin],
            send_sem=col_send.at[piece, target],
            recv_sem=col_recv.at[piece, origin],
            device_id={col_name: target},
            device_id_type=pl.DeviceIdType.MESH,
        )

    for f in range(fields):
        loads[f].wait()
        if f == 0:
            fetches[0].wait()
        high, low = split(
            jnp.concatenate(
                [xin[f, :, z, :] for z in range(share_z)], axis=0
            )
        )
        table = jnp.concatenate([hx[...], hx[...]], axis=0)
        both = jnp.dot(
            jnp.concatenate([high, low], axis=1), table, preferred_element_type=F32
        )
        both = both[:, :nx] + both[:, nx:]
        for group in range(nx // LANES):
            tiles = [
                both[z * share_y : (z + 1) * share_y, group * LANES : (group + 1) * LANES]
                for z in range(share_z)
            ]
            bit = 1
            while bit < share_z:
                keep = (lane & bit) == 0
                for i in range(share_z):
                    if i & bit == 0:
                        a, b = tiles[i], tiles[i + bit]
                        tiles[i] = jnp.where(keep, a, pltpu.roll(b, bit, 1))
                        tiles[i + bit] = jnp.where(keep, pltpu.roll(a, LANES - bit, 1), b)
                bit *= 2
            for i in range(share_z):
                q = group * share_z + i
                target, at = q // quads, q % quads * LANES
                send[f * CUTS + at // wide, target, :, at % wide : at % wide + LANES] = tiles[i]
        if f == 0:
            pl.semaphore_wait(barrier, rows + cols - 2)
        for cut in range(CUTS):
            piece = f * CUTS + cut
            for k in order:
                row_copy(piece, (me + k) % rows, me).start()

    for copy in fetches[1:]:
        copy.start()
    for piece in range(fields * CUTS):
        recv[piece, me] = send[piece, me]
    for copy in fetches[1:]:
        copy.wait()
    tall_x[...] = jnp.broadcast_to(sx[...], (LANES, nx)).T
    tall_y[...] = jnp.broadcast_to(sy[...], (LANES, ny)).T
    part_y = tall_y[pl.ds(my_col * half_y, half_y), :1]
    for x in range(share_x):
        part_x = tall_x[pl.ds(me * share_x + x, 1), :1]
        at = x % width * nz
        scale[x // width, :, at : at + nz] = 1.0 / (part_x + part_y + sz[...])

    for piece in range(fields * CUTS):
        for k in order:
            origin = (me + rows - k) % rows
            row_copy(piece, origin, origin).wait_recv()
        high, low = split(recv[piece].reshape(ny, wide))
        both = jnp.dot(
            hy[...], jnp.concatenate([high, low], axis=0), preferred_element_type=F32
        )
        both = both[:ny] + both[ny:]
        mixed[piece] = both.reshape(cols, half_y, wide)
        for k in range(1, cols):
            col_copy(piece, (my_col + k) % cols, my_col).start()
        lines[piece, my_col] = mixed[piece, my_col]

    for piece in range(fields * CUTS):
        for k in order:
            row_copy(piece, (me + k) % rows, me).wait_send()
        for k in range(1, cols):
            origin = (my_col + cols - k) % cols
            col_copy(piece, origin, origin).wait_recv()
            col_copy(piece, (my_col + k) % cols, my_col).wait_send()


def last_kernel(lines, scale, wz, out, held, out_sem):
    pieces, cols, half_y, wide = lines.shape
    nz = out.shape[3]
    width = scale.shape[2] // nz
    copies = []
    for piece in range(pieces):
        f, cut = piece // CUTS, piece % CUTS
        for i in range(wide // LANES):
            quad = cut * (wide // LANES) + i
            line = jnp.concatenate(
                [lines[piece, c, :, i * LANES : (i + 1) * LANES] for c in range(cols)], axis=1
            )
            high, low = split(line)
            both = jnp.dot(
                jnp.concatenate([high, low], axis=0), wz[0], preferred_element_type=F32
            )
            done = both[:half_y] + both[half_y:]
            done = done + jnp.dot(high, wz[1], preferred_element_type=F32)
            done = done * scale[quad]
            for j in range(width):
                held[f, quad * width + j] = done[:, j * nz : (j + 1) * nz]
            span = pl.ds(quad * width, width)
            copy = pltpu.make_async_copy(held.at[f, span], out.at[f, span], out_sem.at[f, quad])
            copy.start()
            copies.append(copy)
    for copy in copies:
        copy.wait()


def on_device(rows, cols, species, symbol_x, symbol_y, symbol_z):
    fields, nx, share_y, share_z = species.shape
    ny, nz = symbol_y.shape[0], symbol_z.shape[0]
    share_x, half_y = nx // rows, ny // cols
    width = LANES // share_z
    pieces, wide = fields * CUTS, share_x // width * LANES // CUTS
    hx, hy, wz = (jnp.asarray(t) for t in tables(nx, ny, nz, share_z))
    dma = pltpu.SemaphoreType.DMA
    width_z = width * nz
    vmem = pl.BlockSpec(memory_space=pltpu.VMEM)
    lines, scale = pl.pallas_call(
        functools.partial(kernel, rows, cols, ("row", "col")),
        out_shape=(
            jax.ShapeDtypeStruct((pieces, cols, half_y, wide), F32),
            jax.ShapeDtypeStruct((share_x // width, half_y, width_z), F32),
        ),
        in_specs=[pl.BlockSpec(memory_space=pl.ANY)] * 6,
        out_specs=(vmem, vmem),
        scratch_shapes=[
            pltpu.VMEM((fields, share_y, share_z, nx), F32),
            pltpu.VMEM(hx.shape, BF16),
            pltpu.VMEM(hy.shape, BF16),
            pltpu.VMEM((1, nx), F32),
            pltpu.VMEM((1, ny), F32),
            pltpu.VMEM((1, nz), F32),
            pltpu.VMEM((pieces, rows, share_y, wide), F32),
            pltpu.VMEM((pieces, rows, share_y, wide), F32),
            pltpu.VMEM((pieces, cols, half_y, wide), F32),
            pltpu.VMEM((nx, LANES), F32),
            pltpu.VMEM((ny, LANES), F32),
            dma((fields + 5,)),
            dma((pieces, rows)),
            dma((pieces, rows)),
            dma((pieces, cols)),
            dma((pieces, cols)),
        ],
        compiler_params=pltpu.CompilerParams(collective_id=0, has_side_effects=True, vmem_limit_bytes=16 * 2**20),
    )(
        *(pltpu.with_memory_space_constraint(v, pltpu.HBM) for v in (jnp.transpose(species, (0, 2, 3, 1)), hx, hy,
        symbol_x[None, :], symbol_y[None, :], symbol_z[None, :])),
    )
    shape = (fields, share_x, half_y, nz)
    return pl.pallas_call(
        last_kernel,
        out_shape=jax.ShapeDtypeStruct(shape, F32),
        in_specs=[vmem, vmem, vmem],
        out_specs=pl.BlockSpec(memory_space=pl.ANY),
        scratch_shapes=[pltpu.VMEM(shape, F32), dma((fields, share_x // width))],
        compiler_params=pltpu.CompilerParams(vmem_limit_bytes=16 * 2**20),
    )(lines, scale, wz)


def solution(mesh):
    rows, cols = mesh.shape["row"], mesh.shape["col"]
    in_specs = (P(None, None, "row", "col"), P(), P(), P())
    out_specs = P(None, "row", "col", None)
    return jax.shard_map(
        functools.partial(on_device, rows, cols),
        mesh=mesh, in_specs=in_specs, out_specs=out_specs, check_vma=False,
    )
```
